128 devices in a mesh: member: 2 (over core), grid: 64 (over z, y, x).
Axes of the slice: x: 4, y: 4, z: 4, core: 2. Of those that a mesh axis runs over, the one named last changes fastest.
Arguments:
- latent: bfloat16 [4, 131072, 512], P('member', 'grid'), may hold values from -80 to 80
- block_pick: int32 [64, 64], P('grid'), may hold values from 0 to 15
- obs_weight: bfloat16 [64, 64, 32, 128], P('grid'), may hold values from 0.0099487305 to 1
- obs_value: float32 [64, 64, 32, 128], P('grid'), may hold values from -6 to 6
- obs_count: int32 [64, 64], P('grid'), may hold values from 0 to 32, as said below
- w_in: bfloat16 [512, 512], replicated, may hold values from -0.25 to 0.25
- b_in: float32 [512], replicated, may hold values from -3 to 3
- w_out: bfloat16 [512, 128], replicated, may hold values from -0.25 to 0.25
- b_out: float32 [128], replicated, may hold values from -3 to 3
Outputs:
- latent_grad: float32 [4, 131072, 512], P('member', 'grid')
- loss_value: float32 [], replicated
The draws below stay inside these ranges and needn't reach their ends.
Inputs may be any that keep to these rules, and one draw needn't show every extreme that they name: Entry [d, j] counts the live observations of those slots; the live ones are the first slots, k < obs_count[d, j].
All inputs are finite; a program needn't handle non-finite values.
Results may differ from the reference program's by a relative error of at most 0.0041.
Values may be sent and summed in bfloat16 or wider, within the bound.
No kernel may reach another device: no remote copies, remote signals or barrier semaphores. Data moves between devices by JAX's collectives and lax.ppermute only.
A program may use at most 128 MiB of HBM per device.

```python
import math
import jax
import jax.numpy as jnp
from jax import lax

WIDTH = 512
INNER_WIDTH = 512
OBS_CH = 128
BLOCK = 128
POINTS_DEV = 2048
MEMBERS = 4
POINTS = 131072
SLOTS = 32
OBS_ALL = 131072
N_GRID = 64


def draw_obs_count(key, part):
    row_index = jnp.arange(N_GRID, dtype=jnp.int32)
    capacity = jnp.maximum(SLOTS * (N_GRID + 2 * row_index) // (3 * N_GRID - 2), 1)
    lowest = capacity // 2
    spread = jax.random.randint(key, (N_GRID, N_GRID), 0, 1048576, dtype=jnp.int32)
    counts = lowest[:, None] + spread % (capacity - lowest + 1)[:, None]
    diagonal = row_index[:, None] == row_index[None, :]
    return jnp.where(diagonal, capacity[:, None], counts).astype(jnp.int32)


def draw_latent(key, part):
    member_pos = jnp.arange(MEMBERS, dtype=jnp.float32) / (MEMBERS - 1.0)
    sub_key = jax.random.fold_in(key, 7331)
    member_scale = 1.5 * jnp.power(8.0, member_pos)
    base = jnp.clip(jax.random.normal(sub_key, (MEMBERS, POINTS, WIDTH), jnp.float32), -6.0, 6.0)
    return (base * member_scale[:, None, None]).astype(jnp.bfloat16)


def set_ends(entries, rng, low, largest):
    longest = entries.shape.index(max(entries.shape))
    spots = []
    for shift in (0, 1):
        where = [jax.random.randint(jax.random.fold_in(rng, axis), (), 0, length) for axis, length in enumerate(entries.shape)]
        where[longest] = (where[longest] + shift) % entries.shape[longest]
        spots.append(tuple(where))
    return entries.at[spots[0]].set(low).at[spots[1]].set(largest)


def shard_levels(rng, dims, shards, low, largest):
    def one(position, shards_of):
        steps = jax.random.uniform(jax.random.fold_in(jax.random.fold_in(rng, 6), position), (shards_of,), jnp.float32, low / len(shards), largest / len(shards))
        return jnp.repeat(jnp.exp(steps), dims[position] // shards_of).reshape((-1,) + (1,) * (len(dims) - position - 1))

    loudness = one(*shards[0])
    for cut in shards[1:]:
        loudness = loudness * one(*cut)
    return loudness


def bell_draw(key, extent, width, limit, shards=(), held_as=jnp.bfloat16):
    entries = width * jax.random.normal(key, extent, jnp.float32)
    if shards:
        entries = entries * shard_levels(key, extent, shards, -0.22, 0.18)
    return jnp.clip(entries, -limit, limit).astype(held_as)


def setup_inputs(seed: int = 0) -> dict:
    streams_of = jax.random.split(jax.random.key(seed), 10)
    return {
        "latent": draw_latent(jax.random.fold_in(streams_of[9], 71), 0),
        "block_pick": set_ends(jax.random.randint(streams_of[1], (N_GRID, N_GRID), 0, POINTS_DEV // BLOCK), jax.random.fold_in(streams_of[1], 1), 0, (POINTS_DEV // BLOCK) - 1).astype(jnp.int32),
        "obs_weight": jnp.clip(jnp.exp(math.log(1.0) - 4.61031033 * jax.random.uniform(streams_of[2], (N_GRID, N_GRID, SLOTS, BLOCK), jnp.float32) ** shard_levels(streams_of[2], (N_GRID, N_GRID, SLOTS, BLOCK), ((0, 64),), -0.2, 0.2)), 0.0099487305, 1.0).astype(jnp.bfloat16),
        "obs_value": bell_draw(streams_of[3], (N_GRID, N_GRID, SLOTS, OBS_CH), 1.0, 6.0, ((0, 64),), jnp.float32),
        "obs_count": draw_obs_count(jax.random.fold_in(streams_of[9], 71), 0),
        "w_in": bell_draw(streams_of[5], (WIDTH, INNER_WIDTH), WIDTH ** -0.5, 0.25),
        "b_in": bell_draw(streams_of[6], (INNER_WIDTH,), 0.5, 3.0, (), jnp.float32),
        "w_out": bell_draw(streams_of[7], (INNER_WIDTH, OBS_CH), INNER_WIDTH ** -0.5, 0.25),
        "b_out": bell_draw(streams_of[8], (OBS_CH,), 0.5, 3.0, (), jnp.float32),
    }


SOFTEN = 0.1

def smooth_abs(value):
    return jnp.sqrt(value * value + SOFTEN * SOFTEN)

def silu_slope(pre_act):
    sigmoid_value = jax.nn.sigmoid(pre_act)
    return sigmoid_value * (1.0 + pre_act * (1.0 - sigmoid_value))

def reference(latent, block_pick, obs_weight, obs_value, obs_count, w_in, b_in, w_out, b_out):
    block_count = POINTS_DEV // BLOCK
    weight_sum = lax.optimization_barrier(jnp.sum(obs_weight.astype(jnp.float32), axis=3, keepdims=True))
    norm_weight = (obs_weight.astype(jnp.float32) / weight_sum).astype(jnp.bfloat16)
    live_mask = (jnp.arange(SLOTS, dtype=jnp.int32)[None, None, :] < obs_count[:, :, None]).astype(jnp.float32)
    local_blocks = latent.reshape(MEMBERS, N_GRID, block_count, BLOCK, WIDTH)
    owners = jnp.arange(N_GRID, dtype=jnp.int32)

    def forward(owner_index):
        owned = jnp.take(local_blocks, owner_index, axis=1)
        picked_ids = jnp.take(block_pick, owner_index, axis=0).astype(jnp.int32)
        picked = jnp.take(owned, picked_ids, axis=1)
        weights = jnp.take(norm_weight, owner_index, axis=1)
        interp = jnp.einsum('dkp,mdpc->mdkc', weights.astype(jnp.float32), picked.astype(jnp.float32)).astype(jnp.bfloat16)
        pre_act = jnp.einsum('mdkc,ch->mdkh', interp.astype(jnp.float32), w_in.astype(jnp.float32)) + b_in
        hidden = jax.nn.silu(pre_act).astype(jnp.bfloat16)
        predicted = jnp.einsum('mdkh,hv->mdkv', hidden.astype(jnp.float32), w_out.astype(jnp.float32)) + b_out
        target = jnp.take(obs_value, owner_index, axis=1)
        live = jnp.take(live_mask, owner_index, axis=1)
        return (weights, picked_ids, pre_act, predicted, target, live)

    def loss_piece(owner_index):
        outputs = forward(owner_index)
        predicted, target, live = (outputs[3], outputs[4], outputs[5])
        obs_diff = predicted - target[None]
        pair_diff = predicted[:, None] - predicted[None, :]
        per_obs = lax.optimization_barrier(jnp.sum(smooth_abs(obs_diff), axis=0)) / MEMBERS - lax.optimization_barrier(jnp.sum(smooth_abs(pair_diff), axis=(0, 1))) / (2.0 * MEMBERS * (MEMBERS - 1))
        return jnp.sum(per_obs * live[:, :, None])
    loss_sum = jnp.sum(lax.map(loss_piece, owners))
    live_total = jnp.sum(live_mask)
    loss_value = loss_sum / (OBS_CH * live_total)
    grad_scale = OBS_ALL / live_total

    def grad_piece(owner_index):
        weights, picked_ids, pre_act, predicted, target, live = forward(owner_index)
        obs_diff = predicted - target[None]
        pair_diff = predicted[:, None] - predicted[None, :]
        slope_obs = obs_diff / smooth_abs(obs_diff)
        slope_pair = lax.optimization_barrier(jnp.sum(pair_diff / smooth_abs(pair_diff), axis=1))
        grad_pred = (grad_scale * live[None, :, :, None] * (slope_obs / MEMBERS - slope_pair / (MEMBERS * (MEMBERS - 1.0)))).astype(jnp.bfloat16)
        grad_hidden = jnp.einsum('mdkv,hv->mdkh', grad_pred.astype(jnp.float32), w_out.astype(jnp.float32))
        grad_act = (grad_hidden * silu_slope(pre_act)).astype(jnp.bfloat16)
        grad_interp = jnp.einsum('mdkh,ch->mdkc', grad_act.astype(jnp.float32), w_in.astype(jnp.float32)).astype(jnp.bfloat16)
        contribution = jnp.einsum('dkp,mdkc->mdpc', weights.astype(jnp.float32), grad_interp.astype(jnp.float32)).astype(jnp.bfloat16)
        block_onehot = (picked_ids[:, None] == jnp.arange(block_count, dtype=jnp.int32)[None, :]).astype(jnp.float32)
        return jnp.einsum('mdpc,db->mbpc', contribution.astype(jnp.float32), block_onehot)
    grads = lax.map(grad_piece, owners)
    latent_grad = jnp.transpose(grads, (1, 0, 2, 3, 4)).reshape(MEMBERS, POINTS, WIDTH)
    return (latent_grad, loss_value)
```

```python
import functools

import jax
import jax.numpy as jnp
from jax import lax
from jax.experimental import pallas as pl
from jax.experimental.pallas import tpu as pltpu
from jax.sharding import Mesh
from jax.sharding import PartitionSpec as P

GRID = ("grid_0", "grid_1", "grid_2")
SOFTEN = 0.1
GROUP = 8
PARTS = 2


def forward_kernel(picks, latent, weight, w_in, b_in, w_out, b_out, *refs, first):
    predicted, slope, norm, rows = refs[-4:]
    members, _, width = latent.shape
    group, slots, block = weight.shape
    step = pl.program_id(0)
    raw = weight[...].astype(jnp.float32)
    norm[...] = (raw / jnp.sum(raw, axis=2, keepdims=True)).astype(jnp.bfloat16)
    for d in range(group):
        start = pl.multiple_of(picks[first + step * group + d] * block, block)
        for m in range(members):
            rows[m, d] = jnp.dot(
                norm[d],
                latent[m, pl.ds(start, block), :],
                preferred_element_type=jnp.float32,
            ).astype(jnp.bfloat16)
    for m in range(members):
        flat = rows[m].reshape(group * slots, width)
        pre_act = jnp.dot(flat, w_in[...], preferred_element_type=jnp.float32) + b_in[...]
        gate = 0.5 + 0.5 * jnp.tanh(0.5 * pre_act)
        active = pre_act * gate
        slope[m] = (gate + active * (1.0 - gate)).reshape(group, slots, -1)
        out = jnp.dot(
            active.astype(jnp.bfloat16), w_out[...], preferred_element_type=jnp.float32
        )
        predicted[m] = (out + b_out[...]).reshape(group, slots, -1)


def score_kernel(own, other, payload, info, *refs, members_all, scale):
    grad, loss = refs[-2:]
    members, group, slots, channels = own.shape
    step = pl.program_id(0)
    target = payload[:, :slots, :]
    count = payload[:, slots : slots + 1, :]
    slot = lax.broadcasted_iota(jnp.int32, (group, slots, channels), 1).astype(jnp.float32)
    live = (slot < count).astype(jnp.float32)
    live_total = jnp.sum(info[:, 1:2, :], axis=0)
    factor = live * (scale / live_total)[None]

    def soft(value):
        square = value * value + SOFTEN * SOFTEN
        inverse = lax.rsqrt(square)
        return square * inverse, value * inverse

    mine = [own[i] for i in range(members)]
    theirs = [other[i] for i in range(members)]
    own_obs = [soft(v - target) for v in mine]
    other_obs = [soft(v - target) for v in theirs]
    own_pair = soft(mine[0] - mine[1])
    other_pair = soft(theirs[0] - theirs[1])
    cross = [[soft(a - b) for b in theirs] for a in mine]
    obs_sum = (own_obs[0][0] + own_obs[1][0]) + (other_obs[0][0] + other_obs[1][0])
    pair_sum = (own_pair[0] + other_pair[0]) + (
        (cross[0][0][0] + cross[1][1][0]) + (cross[0][1][0] + cross[1][0][0])
    )
    per_obs = obs_sum / members_all - (2.0 * pair_sum + members_all * SOFTEN) / (
        2.0 * members_all * (members_all - 1)
    )
    part = jnp.sum(jnp.sum(per_obs * live, axis=0), axis=0, keepdims=True)

    @pl.when(step == 0)
    def _():
        loss[...] = jnp.zeros_like(loss)

    loss[...] += part
    pair_scale = 1.0 / (members_all * (members_all - 1.0))
    slope_0 = own_pair[1] + cross[0][0][1] + cross[0][1][1]
    slope_1 = cross[1][0][1] + cross[1][1][1] - own_pair[1]
    for i, slope in enumerate((slope_0, slope_1)):
        grad[i] = (factor * (own_obs[i][1] / members_all - slope * pair_scale)).astype(
            jnp.bfloat16
        )


def backward_kernel(picks, grad, slope, norm, w_in, w_out, out, rows):
    members, group, slots, channels = grad.shape
    block = norm.shape[2]
    width = out.shape[2]
    step = pl.program_id(0)

    @pl.when(step == 0)
    def _():
        out[...] = jnp.zeros_like(out)

    for m in range(members):
        flat = grad[m].reshape(group * slots, channels)
        grad_hidden = lax.dot_general(
            flat, w_out[...], (((1,), (1,)), ((), ())), preferred_element_type=jnp.float32
        )
        grad_act = (grad_hidden * slope[m].reshape(group * slots, -1)).astype(jnp.bfloat16)
        grad_interp = lax.dot_general(
            grad_act, w_in[...], (((1,), (1,)), ((), ())), preferred_element_type=jnp.float32
        )
        rows[m] = grad_interp.astype(jnp.bfloat16).reshape(group, slots, width)
    for d in range(group):
        start = pl.multiple_of(picks[step * group + d] * block, block)
        for m in range(members):
            part = lax.dot_general(
                norm[d],
                rows[m, d],
                (((0,), (0,)), ((), ())),
                preferred_element_type=jnp.float32,
            )
            out[m, pl.ds(start, block), :] += part


def whole(shape):
    return pl.BlockSpec(shape, lambda i, *_: (0,) * len(shape))


def forward_call(first, count, picks, latent, weight, w_in, b_in, w_out, b_out, kept):
    members, points, width = latent.shape
    peers, slots, block = weight.shape
    inner, channels = w_out.shape
    start = first // GROUP
    rows = members * count * slots
    return pl.pallas_call(
        functools.partial(forward_kernel, first=first),
        grid_spec=pltpu.PrefetchScalarGridSpec(
            num_scalar_prefetch=1,
            grid=(count // GROUP,),
            in_specs=[
                whole(latent.shape),
                pl.BlockSpec((GROUP, slots, block), lambda i, *_: (start + i, 0, 0)),
                whole(w_in.shape),
                whole(b_in.shape),
                whole(w_out.shape),
                whole(b_out.shape),
            ]
            + [pl.BlockSpec(memory_space=pl.ANY)] * len(kept),
            out_specs=[
                pl.BlockSpec((members, GROUP, slots, channels), lambda i, *_: (0, i, 0, 0)),
                pl.BlockSpec((members, GROUP, slots, inner), lambda i, *_: (0, start + i, 0, 0)),
                pl.BlockSpec((GROUP, slots, block), lambda i, *_: (start + i, 0, 0)),
            ],
            scratch_shapes=[pltpu.VMEM((members, GROUP, slots, width), jnp.bfloat16)],
        ),
        out_shape=[
            jax.ShapeDtypeStruct((members, count, slots, channels), jnp.float32),
            jax.ShapeDtypeStruct((members, peers, slots, inner), jnp.float32),
            jax.ShapeDtypeStruct((peers, slots, block), jnp.bfloat16),
        ],
        input_output_aliases={7 + i: 1 + i for i in range(len(kept))},
        cost_estimate=pl.CostEstimate(
            flops=2 * rows * (block * width + width * inner + inner * channels),
            bytes_accessed=latent.size * 2 + rows * (inner + channels) * 4,
            transcendentals=rows * inner,
        ),
        name="forward",
    )(picks, latent, weight, w_in, b_in, w_out, b_out, *kept)


def score_call(first, own, other, payload, members_all, scale, kept):
    members, count, slots, channels = own.shape
    start = first // GROUP
    rows = members * count * slots
    block = lambda: pl.BlockSpec((members, GROUP, slots, channels), lambda i: (0, i, 0, 0))
    return pl.pallas_call(
        functools.partial(score_kernel, members_all=members_all, scale=scale),
        grid=(count // GROUP,),
        in_specs=[
            block(),
            block(),
            pl.BlockSpec((GROUP, slots + 8, channels), lambda i: (start + i, 0, 0)),
            pl.BlockSpec((payload.shape[0], 8, channels), lambda i: (0, slots // 8, 0)),
        ]
        + [pl.BlockSpec(memory_space=pl.ANY)] * len(kept),
        out_specs=[
            pl.BlockSpec((members, GROUP, slots, channels), lambda i: (0, start + i, 0, 0)),
            pl.BlockSpec((1, channels), lambda i: (0, 0)),
        ],
        out_shape=[
            jax.ShapeDtypeStruct((members, payload.shape[0], slots, channels), jnp.bfloat16),
            jax.ShapeDtypeStruct((1, channels), jnp.float32),
        ],
        input_output_aliases={4 + i: i for i in range(len(kept))},
        cost_estimate=pl.CostEstimate(
            flops=rows * channels * 40,
            bytes_accessed=rows * channels * 12,
            transcendentals=rows * channels * 5,
        ),
        name="score",
    )(own, other, payload, payload, *kept)


def backward_call(picks, grad, slope, norm, w_in, w_out, points):
    members, count, slots, channels = grad.shape
    width, inner = w_in.shape
    block = norm.shape[2]
    rows = members * count * slots
    return pl.pallas_call(
        backward_kernel,
        grid_spec=pltpu.PrefetchScalarGridSpec(
            num_scalar_prefetch=1,
            grid=(count // GROUP,),
            in_specs=[
                pl.BlockSpec((members, GROUP, slots, channels), lambda i, *_: (0, i, 0, 0)),
                pl.BlockSpec((members, GROUP, slots, inner), lambda i, *_: (0, i, 0, 0)),
                pl.BlockSpec((GROUP, slots, block), lambda i, *_: (i, 0, 0)),
                whole(w_in.shape),
                whole(w_out.shape),
            ],
            out_specs=whole((members, points, width)),
            scratch_shapes=[pltpu.VMEM((members, GROUP, slots, width), jnp.bfloat16)],
        ),
        out_shape=jax.ShapeDtypeStruct((members, points, width), jnp.float32),
        cost_estimate=pl.CostEstimate(
            flops=2 * rows * (block * width + width * inner + inner * channels),
            bytes_accessed=members * points * width * 4 + rows * (inner * 4 + channels * 2),
            transcendentals=0,
        ),
        name="backward",
    )(picks, grad, slope, norm, w_in, w_out)


def swap_members(value):
    return lax.ppermute(value, "member", [(0, 1), (1, 0)])


def to_owners(value):
    return lax.all_to_all(value, GRID, split_axis=0, concat_axis=0, tiled=True)


def per_device(latent, block_pick, obs_weight, obs_value, obs_count, w_in, b_in, w_out, b_out):
    members, points, _ = latent.shape
    peers = lax.axis_size(GRID)
    slots, channels = obs_value.shape[2:]
    members_all = members * lax.axis_size("member")
    picks = block_pick[0]
    counts = obs_count[0]
    weight = to_owners(obs_weight[0])
    live_here = jnp.sum(jnp.minimum(counts, slots)).astype(jnp.float32)
    info = jnp.stack(
        [
            jnp.broadcast_to(counts.astype(jnp.float32)[:, None], (peers, channels)),
            jnp.broadcast_to(live_here, (peers, channels)),
        ],
        axis=1,
    )
    info = jnp.pad(info, ((0, 0), (0, 6), (0, 0)))
    payload = to_owners(jnp.concatenate([obs_value[0], info], axis=1))
    count = peers // PARTS
    b_in = b_in[None]
    b_out = b_out[None]
    kept = ()
    predictions = []
    for part in range(PARTS):
        own, *kept = forward_call(
            part * count, count, picks, latent, weight, w_in, b_in, w_out, b_out, kept
        )
        predictions.append((own, swap_members(own)))
    slope, norm = kept
    scale = float(peers * peers * slots)
    grads = ()
    loss_part = 0.0
    for part, (own, other) in enumerate(predictions):
        *grads, loss = score_call(
            part * count, own, other, payload, members_all, scale, grads
        )
        loss_part += jnp.sum(loss)
    loss_all = to_owners(jnp.broadcast_to(loss_part, (peers, 1, 1)))
    live_total = jnp.sum(payload[:, slots + 1, 0])
    loss_value = jnp.sum(loss_all) / (channels * live_total)
    latent_grad = backward_call(picks, grads[0], slope, norm, w_in, w_out, points)
    return latent_grad, loss_value


def solution(mesh):
    split = Mesh(
        mesh.devices.reshape(mesh.shape["member"], 4, 4, 4),
        ("member", "grid_0", "grid_1", "grid_2"),
    )
    return jax.shard_map(
        per_device,
        mesh=split,
        in_specs=(
            P("member", GRID, None),
            P(GRID, None),
            P(GRID, None, None, None),
            P(GRID, None, None, None),
            P(GRID, None),
            P(),
            P(),
            P(),
            P(),
        ),
        out_specs=(P("member", GRID, None), P()),
        check_vma=False,
    )
```

```python
import functools

import jax
import jax.numpy as jnp
from jax import lax
from jax.experimental import pallas as pl
from jax.experimental.pallas import tpu as pltpu
from jax.sharding import Mesh
from jax.sharding import PartitionSpec as P

GRID = ("grid_0", "grid_1", "grid_2")
SOFTEN = 0.1
PARTS = 2
FORWARD_GROUP = 32
SCORE_GROUP = 8


def forward_kernel(
    picks, latent, weight, w_in, b_in, w_out, b_out, predicted, slope, norm, rows, kept, sems, *, first
):
    members, _, width = latent.shape
    _, slots, block = weight.shape
    count = norm.shape[0]
    group = rows.shape[1]
    copies = []
    for begin in range(0, count, group):
        raw = weight[first + begin : first + begin + group].astype(jnp.float32)
        scaled = (raw / jnp.sum(raw, axis=2, keepdims=True)).astype(jnp.bfloat16)
        norm[begin : begin + group] = scaled
        for d in range(group):
            start = pl.multiple_of(picks[first + begin + d] * block, block)
            for m in range(members):
                rows[m, d] = jnp.dot(
                    scaled[d],
                    latent[m, pl.ds(start, block), :],
                    preferred_element_type=jnp.float32,
                ).astype(jnp.bfloat16)
        for m in range(members):
            flat = rows[m].reshape(group * slots, width)
            pre_act = jnp.dot(flat, w_in[...], preferred_element_type=jnp.float32) + b_in[...]
            gate = 0.5 + 0.5 * jnp.tanh(0.5 * pre_act)
            active = pre_act * gate
            kept[m, begin : begin + group] = (
                (gate + active * (1.0 - gate)).astype(jnp.bfloat16).reshape(group, slots, -1)
            )
            copy = pltpu.make_async_copy(
                kept.at[m, begin : begin + group],
                slope.at[m, begin : begin + group],
                sems.at[len(copies)],
            )
            copy.start()
            copies.append(copy)
            out = jnp.dot(
                active.astype(jnp.bfloat16), w_out[...], preferred_element_type=jnp.float32
            )
            predicted[m, begin : begin + group] = (out + b_out[...]).reshape(group, slots, -1)
    for copy in copies:
        copy.wait()


def score_kernel(own, other, payload, previous, grad, loss, *, first, members_all, scale):
    members, count, slots, channels = own.shape
    live_total = jnp.sum(payload[:, slots + 1, :], axis=0, keepdims=True)
    factor = scale / live_total
    slot = lax.broadcasted_iota(jnp.int32, (SCORE_GROUP, slots, channels), 1).astype(jnp.float32)
    obs_scale = 1.0 / members_all
    pair_scale = 1.0 / (members_all * (members_all - 1.0))

    def soft(value):
        square = value * value + SOFTEN * SOFTEN
        inverse = lax.rsqrt(square)
        return square * inverse, value * inverse

    def body(step, total):
        begin = step * SCORE_GROUP
        here = pl.ds(first + begin, SCORE_GROUP)
        target = payload[here, :slots, :]
        live = (slot < payload[here, slots : slots + 1, :]).astype(jnp.float32)
        mine = [own[i, pl.ds(begin, SCORE_GROUP)] for i in range(members)]
        theirs = [other[i, pl.ds(begin, SCORE_GROUP)] for i in range(members)]
        own_obs = [soft(v - target) for v in mine]
        other_obs = [soft(v - target) for v in theirs]
        own_pair = soft(mine[0] - mine[1])
        other_pair = soft(theirs[0] - theirs[1])
        cross = [[soft(a - b) for b in theirs] for a in mine]
        obs_sum = (own_obs[0][0] + own_obs[1][0]) + (other_obs[0][0] + other_obs[1][0])
        pair_sum = (own_pair[0] + other_pair[0]) + (
            (cross[0][0][0] + cross[1][1][0]) + (cross[0][1][0] + cross[1][0][0])
        )
        per_obs = obs_sum * obs_scale - (pair_sum + members_all * SOFTEN * 0.5) * pair_scale
        slope_0 = own_pair[1] + cross[0][0][1] + cross[0][1][1]
        slope_1 = cross[1][0][1] + cross[1][1][1] - own_pair[1]
        size = live * factor[None]
        for i, slope in enumerate((slope_0, slope_1)):
            grad[i, pl.ds(begin, SCORE_GROUP)] = (
                size * (own_obs[i][1] * obs_scale - slope * pair_scale)
            ).astype(jnp.bfloat16)
        return total + jnp.sum((per_obs * live).reshape(-1, 8, channels), axis=0)

    total = lax.fori_loop(0, count // SCORE_GROUP, body, jnp.zeros((8, channels), jnp.float32))
    total = jnp.sum(total, axis=0, keepdims=True)
    if len(loss.shape) == 2:
        loss[...] = previous[...] + total
    else:
        loss[...] = jnp.broadcast_to((previous[...] + total)[None], loss.shape)


def backward_kernel(*refs):
    picks, w_in, w_out = refs[:3]
    grads = refs[3 : 3 + PARTS]
    slopes = refs[3 + PARTS : 3 + 2 * PARTS]
    norms = refs[3 + 2 * PARTS : 3 + 3 * PARTS]
    out, rows, total, grad, slope, norm, out_sem, grad_sem, slope_sem, norm_sem = refs[
        3 + 3 * PARTS :
    ]
    members, count, slots, channels = grads[0].shape
    block = norms[0].shape[2]
    width = total.shape[2]

    def fetch_grad(m, part, ref):
        return pltpu.make_async_copy(
            ref.at[m], grad.at[m * PARTS + part], grad_sem.at[m * PARTS + part]
        )

    def fetch_slope(m, part, ref):
        return pltpu.make_async_copy(
            ref.at[m], slope.at[m * PARTS + part], slope_sem.at[m * PARTS + part]
        )

    def fetch_norm(part, ref):
        return pltpu.make_async_copy(ref, norm.at[part], norm_sem.at[part])

    for m in range(members):
        for part in range(PARTS):
            fetch_grad(m, part, grads[part]).start()
            fetch_slope(m, part, slopes[part]).start()
            if m == 0:
                fetch_norm(part, norms[part]).start()
    total[...] = jnp.zeros(total.shape, total.dtype)
    for part in range(PARTS):
        fetch_norm(part, norms[part]).wait()

    def body(step, carry):
        m = step // PARTS
        part = step % PARTS
        fetch_grad(m, part, grads[0]).wait()
        fetch_slope(m, part, slopes[0]).wait()
        grad_hidden = lax.dot_general(
            grad[step].reshape(count * slots, channels),
            w_out[...],
            (((1,), (1,)), ((), ())),
            preferred_element_type=jnp.float32,
        )
        grad_act = grad_hidden * slope[step].reshape(count * slots, -1).astype(jnp.float32)
        grad_interp = lax.dot_general(
            grad_act.astype(jnp.bfloat16),
            w_in[...],
            (((1,), (1,)), ((), ())),
            preferred_element_type=jnp.float32,
        )
        rows[...] = grad_interp.astype(jnp.bfloat16).reshape(count, slots, width)
        for d in range(count):
            start = pl.multiple_of(picks[part * count + d] * block, block)
            total[m, pl.ds(start, block), :] += lax.dot_general(
                norm[part, d],
                rows[d],
                (((0,), (0,)), ((), ())),
                preferred_element_type=jnp.float32,
            )

        @pl.when(part == PARTS - 1)
        def _():
            pltpu.make_async_copy(total.at[m], out.at[m], out_sem.at[m]).start()

        return carry

    lax.fori_loop(0, members * PARTS, body, 0)
    for m in range(members):
        pltpu.make_async_copy(total.at[m], out.at[m], out_sem.at[m]).wait()


def vmem(count):
    return [pl.BlockSpec(memory_space=pltpu.VMEM)] * count


def hbm(count):
    return [pl.BlockSpec(memory_space=pltpu.HBM)] * count


def smem():
    return [pl.BlockSpec(memory_space=pltpu.SMEM)]


def forward_call(first, count, picks, latent, weight, w_in, b_in, w_out, b_out):
    members, points, width = latent.shape
    _, slots, block = weight.shape
    inner, channels = w_out.shape
    rows = members * count * slots
    return pl.pallas_call(
        functools.partial(forward_kernel, first=first),
        in_specs=smem() + vmem(6),
        out_specs=vmem(1) + hbm(1) + vmem(1),
        scratch_shapes=[
            pltpu.VMEM((members, FORWARD_GROUP, slots, width), jnp.bfloat16),
            pltpu.VMEM((members, count, slots, inner), jnp.bfloat16),
            pltpu.SemaphoreType.DMA((members * count // FORWARD_GROUP,)),
        ],
        out_shape=[
            jax.ShapeDtypeStruct((members, count, slots, channels), jnp.float32),
            jax.ShapeDtypeStruct((members, count, slots, inner), jnp.bfloat16),
            jax.ShapeDtypeStruct((count, slots, block), jnp.bfloat16),
        ],
        compiler_params=pltpu.CompilerParams(vmem_limit_bytes=16 << 20),
        cost_estimate=pl.CostEstimate(
            flops=2 * rows * (block * width + width * inner + inner * channels),
            bytes_accessed=latent.size * 2 + rows * (inner + channels) * 4,
            transcendentals=rows * inner,
        ),
        name="forward",
    )(picks, latent, weight, w_in, b_in, w_out, b_out)


def score_call(first, own, other, payload, previous, loss_shape, members_all, scale):
    members, count, slots, channels = own.shape
    rows = members * count * slots
    return pl.pallas_call(
        functools.partial(score_kernel, first=first, members_all=members_all, scale=scale),
        in_specs=vmem(4),
        out_specs=vmem(2),
        out_shape=[
            jax.ShapeDtypeStruct(own.shape, jnp.bfloat16),
            jax.ShapeDtypeStruct(loss_shape, jnp.float32),
        ],
        compiler_params=pltpu.CompilerParams(vmem_limit_bytes=8 << 20),
        cost_estimate=pl.CostEstimate(
            flops=rows * channels * 40,
            bytes_accessed=rows * channels * 12,
            transcendentals=rows * channels * 5,
        ),
        name="score",
    )(own, other, payload, previous)


def backward_call(picks, grads, slopes, norms, w_in, w_out, points):
    members, count, slots, channels = grads[0].shape
    width, inner = w_in.shape
    block = norms[0].shape[2]
    rows = members * count * slots * PARTS
    return pl.pallas_call(
        backward_kernel,
        in_specs=smem() + vmem(2) + [pl.BlockSpec(memory_space=pl.ANY)] * (3 * PARTS),
        out_specs=pl.BlockSpec(memory_space=pltpu.HBM),
        scratch_shapes=[
            pltpu.VMEM((count, slots, width), jnp.bfloat16),
            pltpu.VMEM((members, points, width), jnp.float32),
            pltpu.VMEM((members * PARTS, count, slots, channels), jnp.bfloat16),
            pltpu.VMEM((members * PARTS, count, slots, inner), jnp.bfloat16),
            pltpu.VMEM((PARTS, count, slots, block), jnp.bfloat16),
            pltpu.SemaphoreType.DMA((members,)),
            pltpu.SemaphoreType.DMA((members * PARTS,)),
            pltpu.SemaphoreType.DMA((members * PARTS,)),
            pltpu.SemaphoreType.DMA((PARTS,)),
        ],
        out_shape=jax.ShapeDtypeStruct((members, points, width), jnp.float32),
        compiler_params=pltpu.CompilerParams(vmem_limit_bytes=32 << 20),
        cost_estimate=pl.CostEstimate(
            flops=2 * rows * (block * width + width * inner + inner * channels),
            bytes_accessed=members * points * width * 4 + rows * (inner * 4 + channels * 2),
            transcendentals=0,
        ),
        name="backward",
    )(picks, w_in, w_out, *grads, *slopes, *norms)


def swap_members(value):
    return lax.ppermute(value, "member", [(0, 1), (1, 0)])


def to_owners(value):
    return lax.all_to_all(value, GRID, split_axis=0, concat_axis=0, tiled=True)


def per_device(latent, block_pick, obs_weight, obs_value, obs_count, w_in, b_in, w_out, b_out):
    members, points, _ = latent.shape
    peers = lax.axis_size(GRID)
    slots, channels = obs_value.shape[2:]
    members_all = members * lax.axis_size("member")
    picks = block_pick[0]
    counts = obs_count[0]
    weight = to_owners(obs_weight[0])
    live_here = jnp.sum(jnp.minimum(counts, slots)).astype(jnp.float32)
    info = jnp.stack(
        [
            jnp.broadcast_to(counts.astype(jnp.float32)[:, None], (peers, channels)),
            jnp.broadcast_to(live_here, (peers, channels)),
        ],
        axis=1,
    )
    info = jnp.pad(info, ((0, 0), (0, 6), (0, 0)))
    payload = to_owners(jnp.concatenate([obs_value[0], info], axis=1))
    count = peers // PARTS
    b_in = b_in[None]
    b_out = b_out[None]
    parts = []
    for part in range(PARTS):
        own, slope, norm = forward_call(
            part * count, count, picks, latent, weight, w_in, b_in, w_out, b_out
        )
        parts.append((own, swap_members(own), slope, norm))
    scale = float(peers * peers * slots)
    grads = []
    loss = jnp.zeros((1, channels), jnp.float32)
    for part, (own, other, _, _) in enumerate(parts):
        loss_shape = (1, channels) if part + 1 < PARTS else (peers, 8, channels)
        grad, loss = score_call(
            part * count, own, other, payload, loss, loss_shape, members_all, scale
        )
        grads.append(grad)
    loss_all = to_owners(loss)
    live_total = jnp.sum(payload[:, slots + 1, 0])
    loss_value = jnp.sum(loss_all[:, 0, :]) / (channels * live_total)
    latent_grad = backward_call(
        picks, grads, [p[2] for p in parts], [p[3] for p in parts], w_in, w_out, points
    )
    return latent_grad, loss_value


def solution(mesh):
    split = Mesh(
        mesh.devices.reshape(mesh.shape["member"], 4, 4, 4),
        ("member", "grid_0", "grid_1", "grid_2"),
    )
    return jax.shard_map(
        per_device,
        mesh=split,
        in_specs=(
            P("member", GRID, None),
            P(GRID, None),
            P(GRID, None, None, None),
            P(GRID, None, None, None),
            P(GRID, None),
            P(),
            P(),
            P(),
            P(),
        ),
        out_specs=(P("member", GRID, None), P()),
        check_vma=False,
    )
```

```python
import functools

import jax
import jax.numpy as jnp
from jax import lax
from jax.experimental import pallas as pl
from jax.experimental.pallas import tpu as pltpu
from jax.sharding import Mesh
from jax.sharding import PartitionSpec as P

GRID = ("grid_0", "grid_1", "grid_2")
SOFTEN = 0.1
HALVES = 2
SCORE_GROUP = 8


def forward_kernel(
    picks,
    latent,
    weight,
    w_in,
    b_in,
    w_out,
    b_out,
    predicted,
    slope,
    norm,
    latent_here,
    weight_here,
    w_in_here,
    rows,
    predicted_here,
    slope_here,
    norm_here,
    latent_sem,
    weight_sem,
    w_in_sem,
    predicted_sem,
    slope_sem,
    norm_sem,
):
    members, _, width = latent.shape
    peers, slots, block = weight.shape
    half = peers // HALVES

    def fetch(m):
        return pltpu.make_async_copy(latent.at[m], latent_here.at[m], latent_sem.at[m])

    def put_predicted(step, m, begin):
        return pltpu.make_async_copy(
            predicted_here.at[step], predicted.at[m, pl.ds(begin, half)], predicted_sem.at[step]
        )

    def put_slope(step, m, begin):
        return pltpu.make_async_copy(
            slope_here.at[step], slope.at[m, pl.ds(begin, half)], slope_sem.at[step]
        )

    fetch_weight = pltpu.make_async_copy(weight, weight_here, weight_sem)
    fetch_w_in = pltpu.make_async_copy(w_in, w_in_here, w_in_sem)
    put_norm = pltpu.make_async_copy(norm_here, norm, norm_sem)
    fetch_weight.start()
    fetch(0).start()
    fetch_w_in.start()
    fetch(1).start()
    fetch_weight.wait()
    raw = weight_here[...].astype(jnp.float32)
    norm_here[...] = (raw / jnp.sum(raw, axis=2, keepdims=True)).astype(jnp.bfloat16)
    put_norm.start()
    fetch_w_in.wait()

    def body(step, carry):
        m = step // HALVES
        begin = (step % HALVES) * half

        @pl.when(step % HALVES == 0)
        def _():
            fetch(m).wait()

        for d in range(half):
            start = pl.multiple_of(picks[begin + d] * block, block)
            rows[d] = jnp.dot(
                norm_here[begin + d],
                latent_here[m, pl.ds(start, block), :],
                preferred_element_type=jnp.float32,
            ).astype(jnp.bfloat16)
        flat = rows[...].reshape(half * slots, width)
        pre_act = jnp.dot(flat, w_in_here[...], preferred_element_type=jnp.float32) + b_in[...]
        gate = 0.5 + 0.5 * jnp.tanh(0.5 * pre_act)
        active = pre_act * gate
        slope_here[step] = (
            (gate + active * (1.0 - gate)).astype(jnp.bfloat16).reshape(half, slots, -1)
        )
        put_slope(step, m, begin).start()
        out = jnp.dot(active.astype(jnp.bfloat16), w_out[...], preferred_element_type=jnp.float32)
        predicted_here[step] = (out + b_out[...]).reshape(half, slots, -1)
        put_predicted(step, m, begin).start()
        return carry

    lax.fori_loop(0, members * HALVES, body, 0)
    put_norm.wait()
    for step in range(members * HALVES):
        put_slope(step, step // HALVES, (step % HALVES) * half).wait()
        put_predicted(step, step // HALVES, (step % HALVES) * half).wait()


def score_kernel(
    own,
    other,
    payload,
    grad,
    loss,
    own_here,
    other_here,
    payload_here,
    grad_here,
    own_sem,
    other_sem,
    payload_sem,
    grad_sem,
    *,
    members_all,
    scale,
):
    members, peers, slots, channels = own.shape
    steps = peers // SCORE_GROUP

    def fetch(source, target, sem, step):
        here = pl.ds(step * SCORE_GROUP, SCORE_GROUP)
        return pltpu.make_async_copy(source.at[:, here], target.at[:, here], sem.at[step])

    fetch_payload = pltpu.make_async_copy(payload, payload_here, payload_sem)
    fetch_payload.start()
    for step in range(steps):
        fetch(own, own_here, own_sem, step).start()
        fetch(other, other_here, other_sem, step).start()
    fetch_payload.wait()
    live_total = jnp.sum(payload_here[:, slots + 1, :], axis=0, keepdims=True)
    factor = scale / live_total
    slot = lax.broadcasted_iota(jnp.int32, (SCORE_GROUP, slots, channels), 1).astype(jnp.float32)
    obs_scale = 1.0 / members_all
    pair_scale = 1.0 / (members_all * (members_all - 1.0))

    def soft(value):
        square = value * value + SOFTEN * SOFTEN
        inverse = lax.rsqrt(square)
        return square * inverse, value * inverse

    def body(step, total):
        here = pl.ds(step * SCORE_GROUP, SCORE_GROUP)
        fetch(own, own_here, own_sem, step).wait()
        fetch(other, other_here, other_sem, step).wait()
        target = payload_here[here, :slots, :]
        live = (slot < payload_here[here, slots : slots + 1, :]).astype(jnp.float32)
        mine = [own_here[i, here] for i in range(members)]
        theirs = [other_here[i, here] for i in range(members)]
        own_obs = [soft(v - target) for v in mine]
        other_obs = [soft(v - target) for v in theirs]
        own_pair = soft(mine[0] - mine[1])
        other_pair = soft(theirs[0] - theirs[1])
        cross = [[soft(a - b) for b in theirs] for a in mine]
        obs_sum = (own_obs[0][0] + own_obs[1][0]) + (other_obs[0][0] + other_obs[1][0])
        pair_sum = (own_pair[0] + other_pair[0]) + (
            (cross[0][0][0] + cross[1][1][0]) + (cross[0][1][0] + cross[1][0][0])
        )
        per_obs = obs_sum * obs_scale - (pair_sum + members_all * SOFTEN * 0.5) * pair_scale
        slope_0 = own_pair[1] + cross[0][0][1] + cross[0][1][1]
        slope_1 = cross[1][0][1] + cross[1][1][1] - own_pair[1]
        size = live * factor[None]
        for i, slope in enumerate((slope_0, slope_1)):
            grad_here[i, here] = (
                size * (own_obs[i][1] * obs_scale - slope * pair_scale)
            ).astype(jnp.bfloat16)
        fetch(grad_here, grad, grad_sem, step).start()
        return total + jnp.sum((per_obs * live).reshape(-1, 8, channels), axis=0)

    total = lax.fori_loop(0, steps, body, jnp.zeros((8, channels), jnp.float32))
    total = jnp.sum(total, axis=0, keepdims=True)
    loss[...] = jnp.broadcast_to(total[None], loss.shape)
    for step in range(steps):
        fetch(grad_here, grad, grad_sem, step).wait()


def backward_kernel(
    picks,
    w_in,
    w_out,
    grad,
    slope,
    norm,
    out,
    w_in_here,
    rows,
    total,
    grad_here,
    slope_here,
    norm_here,
    w_in_sem,
    out_sem,
    grad_sem,
    slope_sem,
    norm_sem,
):
    members, peers, slots, channels = grad.shape
    block = norm.shape[2]
    width = total.shape[2]
    half = peers // HALVES

    def fetch_grad(step, m, begin):
        return pltpu.make_async_copy(
            grad.at[m, pl.ds(begin, half)], grad_here.at[step], grad_sem.at[step]
        )

    def fetch_slope(step, m, begin):
        return pltpu.make_async_copy(
            slope.at[m, pl.ds(begin, half)], slope_here.at[step], slope_sem.at[step]
        )

    def put(m):
        return pltpu.make_async_copy(total.at[m], out.at[m], out_sem.at[m])

    fetch_w_in = pltpu.make_async_copy(w_in, w_in_here, w_in_sem)
    fetch_norm = pltpu.make_async_copy(norm, norm_here, norm_sem)
    for step in range(members * HALVES):
        fetch_grad(step, step // HALVES, (step % HALVES) * half).start()
        fetch_slope(step, step // HALVES, (step % HALVES) * half).start()
        if step == 0:
            fetch_w_in.start()
            fetch_norm.start()
    total[...] = jnp.zeros(total.shape, total.dtype)
    fetch_w_in.wait()
    fetch_norm.wait()

    def body(step, carry):
        m = step // HALVES
        begin = (step % HALVES) * half
        fetch_grad(step, m, begin).wait()
        fetch_slope(step, m, begin).wait()
        grad_hidden = lax.dot_general(
            grad_here[step].reshape(half * slots, channels),
            w_out[...],
            (((1,), (1,)), ((), ())),
            preferred_element_type=jnp.float32,
        )
        grad_act = grad_hidden * slope_here[step].reshape(half * slots, -1).astype(jnp.float32)
        grad_interp = lax.dot_general(
            grad_act.astype(jnp.bfloat16),
            w_in_here[...],
            (((1,), (1,)), ((), ())),
            preferred_element_type=jnp.float32,
        )
        rows[...] = grad_interp.astype(jnp.bfloat16).reshape(half, slots, width)
        for d in range(half):
            start = pl.multiple_of(picks[begin + d] * block, block)
            total[m, pl.ds(start, block), :] += lax.dot_general(
                norm_here[begin + d],
                rows[d],
                (((0,), (0,)), ((), ())),
                preferred_element_type=jnp.float32,
            )

        @pl.when(step % HALVES == HALVES - 1)
        def _():
            put(m).start()

        return carry

    lax.fori_loop(0, members * HALVES, body, 0)
    for m in range(members):
        put(m).wait()


def vmem(count):
    return [pl.BlockSpec(memory_space=pltpu.VMEM)] * count


def smem():
    return [pl.BlockSpec(memory_space=pltpu.SMEM)]


def left(count):
    return [pl.BlockSpec(memory_space=pl.ANY)] * count


def dma(*shape):
    return pltpu.SemaphoreType.DMA(shape) if shape else pltpu.SemaphoreType.DMA


def forward_call(picks, latent, weight, w_in, b_in, w_out, b_out):
    members, _, width = latent.shape
    peers, slots, block = weight.shape
    inner, channels = w_out.shape
    rows = members * peers * slots
    steps = members * HALVES
    half = peers // HALVES
    return pl.pallas_call(
        forward_kernel,
        in_specs=smem() + left(3) + vmem(3),
        out_specs=left(3),
        scratch_shapes=[
            pltpu.VMEM(latent.shape, jnp.bfloat16),
            pltpu.VMEM(weight.shape, jnp.bfloat16),
            pltpu.VMEM(w_in.shape, jnp.bfloat16),
            pltpu.VMEM((half, slots, width), jnp.bfloat16),
            pltpu.VMEM((steps, half, slots, channels), jnp.float32),
            pltpu.VMEM((steps, half, slots, inner), jnp.bfloat16),
            pltpu.VMEM(weight.shape, jnp.bfloat16),
            dma(members),
            dma(),
            dma(),
            dma(steps),
            dma(steps),
            dma(),
        ],
        out_shape=[
            jax.ShapeDtypeStruct((members, peers, slots, channels), jnp.float32),
            jax.ShapeDtypeStruct((members, peers, slots, inner), jnp.bfloat16),
            jax.ShapeDtypeStruct(weight.shape, jnp.bfloat16),
        ],
        cost_estimate=pl.CostEstimate(
            flops=2 * rows * (block * width + width * inner + inner * channels),
            bytes_accessed=latent.size * 2 + rows * (inner * 2 + channels * 4),
            transcendentals=rows * inner,
        ),
        name="forward",
    )(picks, latent, weight, w_in, b_in, w_out, b_out)


def score_call(own, other, payload, members_all, scale):
    members, peers, slots, channels = own.shape
    rows = members * peers * slots
    steps = peers // SCORE_GROUP
    return pl.pallas_call(
        functools.partial(score_kernel, members_all=members_all, scale=scale),
        in_specs=left(3),
        out_specs=left(1) + vmem(1),
        out_shape=[
            jax.ShapeDtypeStruct(own.shape, jnp.bfloat16),
            jax.ShapeDtypeStruct((peers, 8, channels), jnp.float32),
        ],
        scratch_shapes=[
            pltpu.VMEM(own.shape, jnp.float32),
            pltpu.VMEM(own.shape, jnp.float32),
            pltpu.VMEM(payload.shape, jnp.float32),
            pltpu.VMEM(own.shape, jnp.bfloat16),
            dma(steps),
            dma(steps),
            dma(),
            dma(steps),
        ],
        cost_estimate=pl.CostEstimate(
            flops=rows * channels * 40,
            bytes_accessed=rows * channels * 12,
            transcendentals=rows * channels * 5,
        ),
        name="score",
    )(own, other, payload)


def backward_call(picks, grad, slope, norm, w_in, w_out, points):
    members, peers, slots, channels = grad.shape
    width, inner = w_in.shape
    block = norm.shape[2]
    rows = members * peers * slots
    steps = members * HALVES
    half = peers // HALVES
    return pl.pallas_call(
        backward_kernel,
        in_specs=smem() + left(1) + vmem(1) + left(3),
        out_specs=pl.BlockSpec(memory_space=pl.ANY),
        scratch_shapes=[
            pltpu.VMEM(w_in.shape, jnp.bfloat16),
            pltpu.VMEM((half, slots, width), jnp.bfloat16),
            pltpu.VMEM((members, points, width), jnp.float32),
            pltpu.VMEM((steps, half, slots, channels), jnp.bfloat16),
            pltpu.VMEM((steps, half, slots, inner), jnp.bfloat16),
            pltpu.VMEM(norm.shape, jnp.bfloat16),
            dma(),
            dma(members),
            dma(steps),
            dma(steps),
            dma(),
        ],
        out_shape=jax.ShapeDtypeStruct((members, points, width), jnp.float32),
        cost_estimate=pl.CostEstimate(
            flops=2 * rows * (block * width + width * inner + inner * channels),
            bytes_accessed=members * points * width * 4 + rows * (inner * 2 + channels * 2),
            transcendentals=0,
        ),
        name="backward",
    )(picks, w_in, w_out, grad, slope, norm)


def swap_members(value):
    return lax.ppermute(value, "member", [(0, 1), (1, 0)])


def to_owners(value):
    return lax.all_to_all(value, GRID, split_axis=0, concat_axis=0, tiled=True)


def device_step(latent, block_pick, obs_weight, obs_value, obs_count, w_in, b_in, w_out, b_out):
    members, points, _ = latent.shape
    peers = lax.axis_size(GRID)
    slots, channels = obs_value.shape[2:]
    members_all = members * lax.axis_size("member")
    picks = block_pick[0]
    counts = obs_count[0]
    weight = to_owners(obs_weight[0])
    live_here = jnp.sum(jnp.minimum(counts, slots)).astype(jnp.float32)
    info = jnp.stack(
        [
            jnp.broadcast_to(counts.astype(jnp.float32)[:, None], (peers, channels)),
            jnp.broadcast_to(live_here, (peers, channels)),
        ],
        axis=1,
    )
    info = jnp.pad(info, ((0, 0), (0, 6), (0, 0)))
    payload = jnp.concatenate([obs_value[0], info], axis=1)
    payload = to_owners(payload)
    own, slope, norm = forward_call(
        picks, latent, weight, w_in, b_in[None], w_out, b_out[None]
    )
    scale = float(peers * peers * slots)
    grad, loss = score_call(own, swap_members(own), payload, members_all, scale)
    loss_all = to_owners(loss)
    live_total = jnp.sum(payload[:, slots + 1, 0])
    loss_value = jnp.sum(loss_all[:, 0, :]) / (channels * live_total)
    latent_grad = backward_call(picks, grad, slope, norm, w_in, w_out, points)
    return latent_grad, loss_value


def solution(mesh):
    split = Mesh(
        mesh.devices.reshape(mesh.shape["member"], 4, 4, 4),
        ("member", "grid_0", "grid_1", "grid_2"),
    )
    return jax.shard_map(
        device_step,
        mesh=split,
        in_specs=(
            P("member", GRID, None),
            P(GRID, None),
            P(GRID, None, None, None),
            P(GRID, None, None, None),
            P(GRID, None),
            P(),
            P(),
            P(),
            P(),
        ),
        out_specs=(P("member", GRID, None), P()),
        check_vma=False,
    )
```

```python
import functools

import jax
import jax.numpy as jnp
from jax import lax
from jax.experimental import pallas as pl
from jax.experimental.pallas import tpu as pltpu
from jax.sharding import Mesh
from jax.sharding import PartitionSpec as P

GRID = ("grid_0", "grid_1", "grid_2")
SOFTEN = 0.1
HALVES = 2
SCORE_GROUP = 8


def forward_kernel(
    picks,
    latent,
    weight,
    w_in,
    b_in,
    w_out,
    b_out,
    predicted,
    slope,
    norm,
    latent_here,
    weight_here,
    w_in_here,
    rows,
    predicted_here,
    slope_here,
    norm_here,
    latent_sem,
    weight_sem,
    w_in_sem,
    predicted_sem,
    slope_sem,
    norm_sem,
):
    members, _, width = latent.shape
    peers, slots, block = weight.shape
    half = peers // HALVES

    def fetch(m):
        return pltpu.make_async_copy(latent.at[m], latent_here.at[m], latent_sem.at[m])

    def put_predicted(step, m, begin):
        return pltpu.make_async_copy(
            predicted_here.at[step], predicted.at[m, pl.ds(begin, half)], predicted_sem.at[step]
        )

    def put_slope(step, m, begin):
        return pltpu.make_async_copy(
            slope_here.at[step], slope.at[m, pl.ds(begin, half)], slope_sem.at[step]
        )

    fetch_weight = pltpu.make_async_copy(weight, weight_here, weight_sem)
    fetch_w_in = pltpu.make_async_copy(w_in, w_in_here, w_in_sem)
    put_norm = pltpu.make_async_copy(norm_here, norm, norm_sem)
    fetch_weight.start()
    fetch(0).start()
    fetch_w_in.start()
    fetch(1).start()
    fetch_weight.wait()
    raw = weight_here[...].astype(jnp.float32)
    norm_here[...] = (raw / jnp.sum(raw, axis=2, keepdims=True)).astype(jnp.bfloat16)
    put_norm.start()
    fetch_w_in.wait()

    def body(step, carry):
        m = step // HALVES
        begin = (step % HALVES) * half

        @pl.when(step % HALVES == 0)
        def _():
            fetch(m).wait()

        for d in range(half):
            start = pl.multiple_of(picks[begin + d] * block, block)
            rows[d] = jnp.dot(
                norm_here[begin + d],
                latent_here[m, pl.ds(start, block), :],
                preferred_element_type=jnp.float32,
            ).astype(jnp.bfloat16)
        flat = rows[...].reshape(half * slots, width)
        pre_act = jnp.dot(flat, w_in_here[...], preferred_element_type=jnp.float32) + b_in[...]
        gate = 0.5 + 0.5 * jnp.tanh(0.5 * pre_act)
        active = pre_act * gate
        slope_here[step] = (
            (gate + active * (1.0 - gate)).astype(jnp.bfloat16).reshape(half, slots, -1)
        )
        put_slope(step, m, begin).start()
        out = jnp.dot(active.astype(jnp.bfloat16), w_out[...], preferred_element_type=jnp.float32)
        predicted_here[step] = (out + b_out[...]).reshape(half, slots, -1)
        put_predicted(step, m, begin).start()
        return carry

    lax.fori_loop(0, members * HALVES, body, 0)
    put_norm.wait()
    for step in range(members * HALVES):
        put_slope(step, step // HALVES, (step % HALVES) * half).wait()
        put_predicted(step, step // HALVES, (step % HALVES) * half).wait()


def score_kernel(
    member,
    own,
    other,
    payload,
    payload_other,
    grad,
    loss,
    own_here,
    other_here,
    payload_here,
    grad_here,
    own_sem,
    other_sem,
    payload_sem,
    grad_sem,
    *,
    members_all,
    scale,
):
    members, peers, slots, channels = own.shape
    steps = peers // SCORE_GROUP

    def fetch(source, target, sem, step):
        here = pl.ds(step * SCORE_GROUP, SCORE_GROUP)
        return pltpu.make_async_copy(source.at[:, here], target.at[:, here], sem.at[step])

    share = payload.shape[1] - 8

    def fetch_values(source, position, sem):
        first = pl.multiple_of(position * share, 8)
        return pltpu.make_async_copy(
            source.at[:, pl.ds(0, share)],
            payload_here.at[:, pl.ds(first, share)],
            payload_sem.at[sem],
        )

    me = member[0]
    fetch_info = pltpu.make_async_copy(
        payload.at[:, pl.ds(share, 8)], payload_here.at[:, pl.ds(slots, 8)], payload_sem.at[2]
    )
    fetch_info.start()
    fetch_values(payload, me, 0).start()
    fetch_values(payload_other, 1 - me, 1).start()
    for step in range(steps):
        fetch(own, own_here, own_sem, step).start()
        fetch(other, other_here, other_sem, step).start()
    fetch_info.wait()
    live_total = jnp.sum(payload_here[:, slots + 1, :], axis=0, keepdims=True)
    factor = scale / live_total
    slot = lax.broadcasted_iota(jnp.int32, (SCORE_GROUP, slots, channels), 1).astype(jnp.float32)
    obs_scale = 1.0 / members_all
    pair_scale = 1.0 / (members_all * (members_all - 1.0))
    fetch_values(payload, me, 0).wait()
    fetch_values(payload_other, 1 - me, 1).wait()

    def soft(value):
        square = value * value + SOFTEN * SOFTEN
        inverse = lax.rsqrt(square)
        return square * inverse, value * inverse

    def body(step, total):
        here = pl.ds(step * SCORE_GROUP, SCORE_GROUP)
        fetch(own, own_here, own_sem, step).wait()
        fetch(other, other_here, other_sem, step).wait()
        target = payload_here[here, :slots, :]
        live = (slot < payload_here[here, slots : slots + 1, :]).astype(jnp.float32)
        mine = [own_here[i, here] for i in range(members)]
        theirs = [other_here[i, here] for i in range(members)]
        own_obs = [soft(v - target) for v in mine]
        other_obs = [soft(v - target) for v in theirs]
        own_pair = soft(mine[0] - mine[1])
        other_pair = soft(theirs[0] - theirs[1])
        cross = [[soft(a - b) for b in theirs] for a in mine]
        obs_sum = (own_obs[0][0] + own_obs[1][0]) + (other_obs[0][0] + other_obs[1][0])
        pair_sum = (own_pair[0] + other_pair[0]) + (
            (cross[0][0][0] + cross[1][1][0]) + (cross[0][1][0] + cross[1][0][0])
        )
        per_obs = obs_sum * obs_scale - (pair_sum + members_all * SOFTEN * 0.5) * pair_scale
        slope_0 = own_pair[1] + cross[0][0][1] + cross[0][1][1]
        slope_1 = cross[1][0][1] + cross[1][1][1] - own_pair[1]
        size = live * factor[None]
        for i, slope in enumerate((slope_0, slope_1)):
            grad_here[i, here] = (
                size * (own_obs[i][1] * obs_scale - slope * pair_scale)
            ).astype(jnp.bfloat16)
        fetch(grad_here, grad, grad_sem, step).start()
        return total + jnp.sum((per_obs * live).reshape(-1, 8, channels), axis=0)

    total = lax.fori_loop(0, steps, body, jnp.zeros((8, channels), jnp.float32))
    total = jnp.sum(total, axis=0, keepdims=True)
    row = lax.broadcasted_iota(jnp.int32, loss.shape, 1)
    loss[...] = jnp.where(row == 0, total[None], live_total[None])
    for step in range(steps):
        fetch(grad_here, grad, grad_sem, step).wait()


def backward_kernel(
    picks,
    w_in,
    w_out,
    grad,
    slope,
    norm,
    out,
    w_in_here,
    rows,
    total,
    grad_here,
    slope_here,
    norm_here,
    w_in_sem,
    out_sem,
    grad_sem,
    slope_sem,
    norm_sem,
):
    members, peers, slots, channels = grad.shape
    block = norm.shape[2]
    width = total.shape[2]
    half = peers // HALVES

    def fetch_grad(step, m, begin):
        return pltpu.make_async_copy(
            grad.at[m, pl.ds(begin, half)], grad_here.at[step], grad_sem.at[step]
        )

    def fetch_slope(step, m, begin):
        return pltpu.make_async_copy(
            slope.at[m, pl.ds(begin, half)], slope_here.at[step], slope_sem.at[step]
        )

    def put(m):
        return pltpu.make_async_copy(total.at[m], out.at[m], out_sem.at[m])

    fetch_w_in = pltpu.make_async_copy(w_in, w_in_here, w_in_sem)
    fetch_norm = pltpu.make_async_copy(norm, norm_here, norm_sem)
    for step in range(members * HALVES):
        fetch_grad(step, step // HALVES, (step % HALVES) * half).start()
        fetch_slope(step, step // HALVES, (step % HALVES) * half).start()
        if step == 0:
            fetch_w_in.start()
            fetch_norm.start()
    total[...] = jnp.zeros(total.shape, total.dtype)
    fetch_w_in.wait()
    fetch_norm.wait()

    def body(step, carry):
        m = step // HALVES
        begin = (step % HALVES) * half
        fetch_grad(step, m, begin).wait()
        fetch_slope(step, m, begin).wait()
        grad_hidden = lax.dot_general(
            grad_here[step].reshape(half * slots, channels),
            w_out[...],
            (((1,), (1,)), ((), ())),
            preferred_element_type=jnp.float32,
        )
        grad_act = grad_hidden * slope_here[step].reshape(half * slots, -1).astype(jnp.float32)
        grad_interp = lax.dot_general(
            grad_act.astype(jnp.bfloat16),
            w_in_here[...],
            (((1,), (1,)), ((), ())),
            preferred_element_type=jnp.float32,
        )
        rows[...] = grad_interp.astype(jnp.bfloat16).reshape(half, slots, width)
        for d in range(half):
            start = pl.multiple_of(picks[begin + d] * block, block)
            total[m, pl.ds(start, block), :] += lax.dot_general(
                norm_here[begin + d],
                rows[d],
                (((0,), (0,)), ((), ())),
                preferred_element_type=jnp.float32,
            )

        @pl.when(step % HALVES == HALVES - 1)
        def _():
            put(m).start()

        return carry

    lax.fori_loop(0, members * HALVES, body, 0)
    for m in range(members):
        put(m).wait()


def vmem(count):
    return [pl.BlockSpec(memory_space=pltpu.VMEM)] * count


def smem():
    return [pl.BlockSpec(memory_space=pltpu.SMEM)]


def left(count):
    return [pl.BlockSpec(memory_space=pl.ANY)] * count


def dma(*shape):
    return pltpu.SemaphoreType.DMA(shape) if shape else pltpu.SemaphoreType.DMA


def forward_call(picks, latent, weight, w_in, b_in, w_out, b_out):
    members, _, width = latent.shape
    peers, slots, block = weight.shape
    inner, channels = w_out.shape
    rows = members * peers * slots
    steps = members * HALVES
    half = peers // HALVES
    return pl.pallas_call(
        forward_kernel,
        in_specs=smem() + left(3) + vmem(3),
        out_specs=left(3),
        scratch_shapes=[
            pltpu.VMEM(latent.shape, jnp.bfloat16),
            pltpu.VMEM(weight.shape, jnp.bfloat16),
            pltpu.VMEM(w_in.shape, jnp.bfloat16),
            pltpu.VMEM((half, slots, width), jnp.bfloat16),
            pltpu.VMEM((steps, half, slots, channels), jnp.float32),
            pltpu.VMEM((steps, half, slots, inner), jnp.bfloat16),
            pltpu.VMEM(weight.shape, jnp.bfloat16),
            dma(members),
            dma(),
            dma(),
            dma(steps),
            dma(steps),
            dma(),
        ],
        out_shape=[
            jax.ShapeDtypeStruct((members, peers, slots, channels), jnp.float32),
            jax.ShapeDtypeStruct((members, peers, slots, inner), jnp.bfloat16),
            jax.ShapeDtypeStruct(weight.shape, jnp.bfloat16),
        ],
        cost_estimate=pl.CostEstimate(
            flops=2 * rows * (block * width + width * inner + inner * channels),
            bytes_accessed=latent.size * 2 + rows * (inner * 2 + channels * 4),
            transcendentals=rows * inner,
        ),
        name="forward",
    )(picks, latent, weight, w_in, b_in, w_out, b_out)


def score_call(member, own, other, payload, payload_other, members_all, scale):
    members, peers, slots, channels = own.shape
    rows = members * peers * slots
    steps = peers // SCORE_GROUP
    return pl.pallas_call(
        functools.partial(score_kernel, members_all=members_all, scale=scale),
        in_specs=smem() + left(4),
        out_specs=left(1) + vmem(1),
        out_shape=[
            jax.ShapeDtypeStruct(own.shape, jnp.bfloat16),
            jax.ShapeDtypeStruct((peers, 8, channels), jnp.float32),
        ],
        scratch_shapes=[
            pltpu.VMEM(own.shape, jnp.float32),
            pltpu.VMEM(own.shape, jnp.float32),
            pltpu.VMEM((peers, slots + 8, channels), jnp.float32),
            pltpu.VMEM(own.shape, jnp.bfloat16),
            dma(steps),
            dma(steps),
            dma(3),
            dma(steps),
        ],
        cost_estimate=pl.CostEstimate(
            flops=rows * channels * 40,
            bytes_accessed=rows * channels * 12,
            transcendentals=rows * channels * 5,
        ),
        name="score",
    )(member, own, other, payload, payload_other)


def backward_call(picks, grad, slope, norm, w_in, w_out, points):
    members, peers, slots, channels = grad.shape
    width, inner = w_in.shape
    block = norm.shape[2]
    rows = members * peers * slots
    steps = members * HALVES
    half = peers // HALVES
    return pl.pallas_call(
        backward_kernel,
        in_specs=smem() + left(1) + vmem(1) + left(3),
        out_specs=pl.BlockSpec(memory_space=pl.ANY),
        scratch_shapes=[
            pltpu.VMEM(w_in.shape, jnp.bfloat16),
            pltpu.VMEM((half, slots, width), jnp.bfloat16),
            pltpu.VMEM((members, points, width), jnp.float32),
            pltpu.VMEM((steps, half, slots, channels), jnp.bfloat16),
            pltpu.VMEM((steps, half, slots, inner), jnp.bfloat16),
            pltpu.VMEM(norm.shape, jnp.bfloat16),
            dma(),
            dma(members),
            dma(steps),
            dma(steps),
            dma(),
        ],
        out_shape=jax.ShapeDtypeStruct((members, points, width), jnp.float32),
        cost_estimate=pl.CostEstimate(
            flops=2 * rows * (block * width + width * inner + inner * channels),
            bytes_accessed=members * points * width * 4 + rows * (inner * 2 + channels * 2),
            transcendentals=0,
        ),
        name="backward",
    )(picks, w_in, w_out, grad, slope, norm)


def swap_members(value):
    return lax.ppermute(value, "member", [(0, 1), (1, 0)])


def to_owners(value):
    return lax.all_to_all(value, GRID, split_axis=0, concat_axis=0, tiled=True)


def device_step(latent, block_pick, obs_weight, obs_value, obs_count, w_in, b_in, w_out, b_out):
    members, points, _ = latent.shape
    peers = lax.axis_size(GRID)
    slots, channels = obs_value.shape[2:]
    members_all = members * lax.axis_size("member")
    picks = block_pick[0]
    counts = obs_count[0]
    weight = to_owners(obs_weight[0])
    live_here = jnp.sum(jnp.minimum(counts, slots)).astype(jnp.float32)
    info = jnp.stack(
        [
            jnp.broadcast_to(counts.astype(jnp.float32)[:, None], (peers, channels)),
            jnp.broadcast_to(live_here, (peers, channels)),
        ],
        axis=1,
    )
    info = jnp.pad(info, ((0, 0), (0, 6), (0, 0)))
    member = lax.axis_index("member")
    share = slots // lax.axis_size("member")
    values = lax.dynamic_slice_in_dim(obs_value[0], member * share, share, axis=1)
    payload = jnp.concatenate([values, info], axis=1)
    payload = to_owners(payload)
    own, slope, norm = forward_call(
        picks, latent, weight, w_in, b_in[None], w_out, b_out[None]
    )
    scale = float(peers * peers * slots)
    grad, loss = score_call(
        jnp.full((1,), member, jnp.int32),
        own,
        swap_members(own),
        payload,
        swap_members(payload),
        members_all,
        scale,
    )
    loss_all = to_owners(loss)
    loss_value = jnp.sum(loss_all[:, 0, :]) / (channels * loss_all[0, 1, 0])
    latent_grad = backward_call(picks, grad, slope, norm, w_in, w_out, points)
    return latent_grad, loss_value


def solution(mesh):
    split = Mesh(
        mesh.devices.reshape(mesh.shape["member"], 4, 4, 4),
        ("member", "grid_0", "grid_1", "grid_2"),
    )
    return jax.shard_map(
        device_step,
        mesh=split,
        in_specs=(
            P("member", GRID, None),
            P(GRID, None),
            P(GRID, None, None, None),
            P(GRID, None, None, None),
            P(GRID, None),
            P(),
            P(),
            P(),
            P(),
        ),
        out_specs=(P("member", GRID, None), P()),
        check_vma=False,
    )
```

```python
import functools

import jax
import jax.numpy as jnp
from jax import lax
from jax.experimental import pallas as pl
from jax.experimental.pallas import tpu as pltpu
from jax.sharding import Mesh
from jax.sharding import PartitionSpec as P

GRID = ("grid_0", "grid_1", "grid_2")
SOFTEN = 0.1
HALVES = 2
SCORE_GROUP = 8


def forward_kernel(
    picks,
    latent,
    weight,
    w_in,
    b_in,
    w_out,
    b_out,
    predicted,
    slope,
    norm,
    latent_here,
    weight_here,
    w_in_here,
    rows,
    predicted_here,
    slope_here,
    norm_here,
    latent_sem,
    weight_sem,
    w_in_sem,
    predicted_sem,
    slope_sem,
    norm_sem,
):
    members, _, width = latent.shape
    peers, slots, block = weight.shape
    half = peers // HALVES

    def fetch(m):
        return pltpu.make_async_copy(latent.at[m], latent_here.at[m], latent_sem.at[m])

    def put_predicted(step, m, begin):
        return pltpu.make_async_copy(
            predicted_here.at[step], predicted.at[m, pl.ds(begin, half)], predicted_sem.at[step]
        )

    def put_slope(step, m, begin):
        return pltpu.make_async_copy(
            slope_here.at[step], slope.at[m, pl.ds(begin, half)], slope_sem.at[step]
        )

    fetch_weight = pltpu.make_async_copy(weight, weight_here, weight_sem)
    fetch_w_in = pltpu.make_async_copy(w_in, w_in_here, w_in_sem)
    put_norm = pltpu.make_async_copy(norm_here, norm, norm_sem)
    fetch_weight.start()
    fetch(0).start()
    fetch_w_in.start()
    fetch(1).start()
    fetch_weight.wait()
    raw = weight_here[...].astype(jnp.float32)
    norm_here[...] = (raw / jnp.sum(raw, axis=2, keepdims=True)).astype(jnp.bfloat16)
    put_norm.start()
    fetch_w_in.wait()

    def body(step, carry):
        m = step // HALVES
        begin = (step % HALVES) * half

        @pl.when(step % HALVES == 0)
        def _():
            fetch(m).wait()

        for d in range(half):
            start = pl.multiple_of(picks[begin + d] * block, block)
            rows[d] = jnp.dot(
                norm_here[begin + d],
                latent_here[m, pl.ds(start, block), :],
                preferred_element_type=jnp.float32,
            ).astype(jnp.bfloat16)
        flat = rows[...].reshape(half * slots, width)
        pre_act = jnp.dot(flat, w_in_here[...], preferred_element_type=jnp.float32) + b_in[...]
        gate = 0.5 + 0.5 * jnp.tanh(0.5 * pre_act)
        active = pre_act * gate
        slope_here[step] = (
            (gate + active * (1.0 - gate)).astype(jnp.bfloat16).reshape(half, slots, -1)
        )
        put_slope(step, m, begin).start()
        out = jnp.dot(active.astype(jnp.bfloat16), w_out[...], preferred_element_type=jnp.float32)
        predicted_here[step] = (out + b_out[...]).reshape(half, slots, -1)
        put_predicted(step, m, begin).start()
        return carry

    lax.fori_loop(0, members * HALVES, body, 0)
    put_norm.wait()
    for step in range(members * HALVES):
        put_slope(step, step // HALVES, (step % HALVES) * half).wait()
        put_predicted(step, step // HALVES, (step % HALVES) * half).wait()


def score_kernel(
    own,
    other,
    payload,
    grad,
    loss,
    own_here,
    other_here,
    payload_here,
    grad_here,
    own_sem,
    other_sem,
    payload_sem,
    grad_sem,
    *,
    members_all,
    scale,
):
    members, peers, slots, channels = own.shape
    steps = peers // SCORE_GROUP

    def fetch(source, target, sem, step):
        here = pl.ds(step * SCORE_GROUP, SCORE_GROUP)
        return pltpu.make_async_copy(source.at[:, here], target.at[:, here], sem.at[step])

    fetch_payload = pltpu.make_async_copy(payload, payload_here, payload_sem)
    fetch_payload.start()
    for step in range(steps):
        fetch(own, own_here, own_sem, step).start()
        fetch(other, other_here, other_sem, step).start()
    fetch_payload.wait()
    live_total = jnp.sum(payload_here[:, slots + 1, :], axis=0, keepdims=True)
    factor = scale / live_total
    slot = lax.broadcasted_iota(jnp.int32, (SCORE_GROUP, slots, channels), 1).astype(jnp.float32)
    obs_scale = 1.0 / members_all
    pair_scale = 1.0 / (members_all * (members_all - 1.0))

    def soft(value):
        square = value * value + SOFTEN * SOFTEN
        inverse = lax.rsqrt(square)
        return square * inverse, value * inverse

    def body(step, total):
        here = pl.ds(step * SCORE_GROUP, SCORE_GROUP)
        fetch(own, own_here, own_sem, step).wait()
        fetch(other, other_here, other_sem, step).wait()
        target = payload_here[here, :slots, :]
        live = (slot < payload_here[here, slots : slots + 1, :]).astype(jnp.float32)
        mine = [own_here[i, here] for i in range(members)]
        theirs = [other_here[i, here] for i in range(members)]
        own_obs = [soft(v - target) for v in mine]
        other_obs = [soft(v - target) for v in theirs]
        own_pair = soft(mine[0] - mine[1])
        other_pair = soft(theirs[0] - theirs[1])
        cross = [[soft(a - b) for b in theirs] for a in mine]
        obs_sum = (own_obs[0][0] + own_obs[1][0]) + (other_obs[0][0] + other_obs[1][0])
        pair_sum = (own_pair[0] + other_pair[0]) + (
            (cross[0][0][0] + cross[1][1][0]) + (cross[0][1][0] + cross[1][0][0])
        )
        per_obs = obs_sum * obs_scale - (pair_sum + members_all * SOFTEN * 0.5) * pair_scale
        slope_0 = own_pair[1] + cross[0][0][1] + cross[0][1][1]
        slope_1 = cross[1][0][1] + cross[1][1][1] - own_pair[1]
        size = live * factor[None]
        for i, slope in enumerate((slope_0, slope_1)):
            grad_here[i, here] = (
                size * (own_obs[i][1] * obs_scale - slope * pair_scale)
            ).astype(jnp.bfloat16)
        fetch(grad_here, grad, grad_sem, step).start()
        return total + jnp.sum((per_obs * live).reshape(-1, 8, channels), axis=0)

    total = lax.fori_loop(0, steps, body, jnp.zeros((8, channels), jnp.float32))
    total = jnp.sum(total, axis=0, keepdims=True) / (channels * live_total)
    loss[...] = jnp.broadcast_to(total[None], loss.shape)
    for step in range(steps):
        fetch(grad_here, grad, grad_sem, step).wait()


def backward_kernel(
    picks,
    w_in,
    w_out,
    grad,
    slope,
    norm,
    out,
    w_in_here,
    rows,
    total,
    grad_here,
    slope_here,
    norm_here,
    w_in_sem,
    out_sem,
    grad_sem,
    slope_sem,
    norm_sem,
):
    members, peers, slots, channels = grad.shape
    block = norm.shape[2]
    width = total.shape[2]
    half = peers // HALVES

    def fetch_grad(step, m, begin):
        return pltpu.make_async_copy(
            grad.at[m, pl.ds(begin, half)], grad_here.at[step], grad_sem.at[step]
        )

    def fetch_slope(step, m, begin):
        return pltpu.make_async_copy(
            slope.at[m, pl.ds(begin, half)], slope_here.at[step], slope_sem.at[step]
        )

    part_width = width // HALVES

    def put(m, part):
        columns = pl.ds(part * part_width, part_width)
        return pltpu.make_async_copy(
            total.at[m, :, columns], out.at[m, :, columns], out_sem.at[m, part]
        )

    fetch_w_in = pltpu.make_async_copy(w_in, w_in_here, w_in_sem)
    fetch_norm = pltpu.make_async_copy(norm, norm_here, norm_sem)
    for step in range(members * HALVES):
        fetch_grad(step, step // HALVES, (step % HALVES) * half).start()
        fetch_slope(step, step // HALVES, (step % HALVES) * half).start()
        if step == 0:
            fetch_w_in.start()
            fetch_norm.start()
    total[...] = jnp.zeros(total.shape, total.dtype)
    fetch_w_in.wait()
    fetch_norm.wait()

    def body(step, carry):
        m = step // HALVES
        begin = (step % HALVES) * half
        fetch_grad(step, m, begin).wait()
        fetch_slope(step, m, begin).wait()
        grad_hidden = lax.dot_general(
            grad_here[step].reshape(half * slots, channels),
            w_out[...],
            (((1,), (1,)), ((), ())),
            preferred_element_type=jnp.float32,
        )
        grad_act = grad_hidden * slope_here[step].reshape(half * slots, -1).astype(jnp.float32)
        grad_interp = lax.dot_general(
            grad_act.astype(jnp.bfloat16),
            w_in_here[...],
            (((1,), (1,)), ((), ())),
            preferred_element_type=jnp.float32,
        )
        rows[...] = grad_interp.astype(jnp.bfloat16).reshape(half, slots, width)
        for part in range(HALVES):
            columns = pl.ds(part * part_width, part_width)
            for d in range(half):
                start = pl.multiple_of(picks[begin + d] * block, block)
                total[m, pl.ds(start, block), columns] += lax.dot_general(
                    norm_here[begin + d],
                    rows[d, :, columns],
                    (((0,), (0,)), ((), ())),
                    preferred_element_type=jnp.float32,
                )

            @pl.when(step % HALVES == HALVES - 1)
            def _(part=part):
                put(m, part).start()

        return carry

    lax.fori_loop(0, members * HALVES, body, 0)
    for m in range(members):
        for part in range(HALVES):
            put(m, part).wait()


def vmem(count):
    return [pl.BlockSpec(memory_space=pltpu.VMEM)] * count


def smem():
    return [pl.BlockSpec(memory_space=pltpu.SMEM)]


def left(count):
    return [pl.BlockSpec(memory_space=pl.ANY)] * count


def dma(*shape):
    return pltpu.SemaphoreType.DMA(shape) if shape else pltpu.SemaphoreType.DMA


def forward_call(picks, latent, weight, w_in, b_in, w_out, b_out):
    members, _, width = latent.shape
    peers, slots, block = weight.shape
    inner, channels = w_out.shape
    rows = members * peers * slots
    steps = members * HALVES
    half = peers // HALVES
    return pl.pallas_call(
        forward_kernel,
        in_specs=smem() + left(3) + vmem(3),
        out_specs=left(3),
        scratch_shapes=[
            pltpu.VMEM(latent.shape, jnp.bfloat16),
            pltpu.VMEM(weight.shape, jnp.bfloat16),
            pltpu.VMEM(w_in.shape, jnp.bfloat16),
            pltpu.VMEM((half, slots, width), jnp.bfloat16),
            pltpu.VMEM((steps, half, slots, channels), jnp.float32),
            pltpu.VMEM((steps, half, slots, inner), jnp.bfloat16),
            pltpu.VMEM(weight.shape, jnp.bfloat16),
            dma(members),
            dma(),
            dma(),
            dma(steps),
            dma(steps),
            dma(),
        ],
        out_shape=[
            jax.ShapeDtypeStruct((members, peers, slots, channels), jnp.float32),
            jax.ShapeDtypeStruct((members, peers, slots, inner), jnp.bfloat16),
            jax.ShapeDtypeStruct(weight.shape, jnp.bfloat16),
        ],
        cost_estimate=pl.CostEstimate(
            flops=2 * rows * (block * width + width * inner + inner * channels),
            bytes_accessed=latent.size * 2 + rows * (inner * 2 + channels * 4),
            transcendentals=rows * inner,
        ),
        name="forward",
    )(picks, latent, weight, w_in, b_in, w_out, b_out)


def score_call(own, other, payload, members_all, scale):
    members, peers, slots, channels = own.shape
    rows = members * peers * slots
    steps = peers // SCORE_GROUP
    return pl.pallas_call(
        functools.partial(score_kernel, members_all=members_all, scale=scale),
        in_specs=left(3),
        out_specs=left(1) + vmem(1),
        out_shape=[
            jax.ShapeDtypeStruct(own.shape, jnp.bfloat16),
            jax.ShapeDtypeStruct((peers, 8, channels), jnp.float32),
        ],
        scratch_shapes=[
            pltpu.VMEM(own.shape, jnp.float32),
            pltpu.VMEM(own.shape, jnp.float32),
            pltpu.VMEM(payload.shape, jnp.float32),
            pltpu.VMEM(own.shape, jnp.bfloat16),
            dma(steps),
            dma(steps),
            dma(),
            dma(steps),
        ],
        cost_estimate=pl.CostEstimate(
            flops=rows * channels * 40,
            bytes_accessed=rows * channels * 12,
            transcendentals=rows * channels * 5,
        ),
        name="score",
    )(own, other, payload)


def backward_call(picks, grad, slope, norm, w_in, w_out, points):
    members, peers, slots, channels = grad.shape
    width, inner = w_in.shape
    block = norm.shape[2]
    rows = members * peers * slots
    steps = members * HALVES
    half = peers // HALVES
    return pl.pallas_call(
        backward_kernel,
        in_specs=smem() + left(1) + vmem(1) + left(3),
        out_specs=pl.BlockSpec(memory_space=pl.ANY),
        scratch_shapes=[
            pltpu.VMEM(w_in.shape, jnp.bfloat16),
            pltpu.VMEM((half, slots, width), jnp.bfloat16),
            pltpu.VMEM((members, points, width), jnp.float32),
            pltpu.VMEM((steps, half, slots, channels), jnp.bfloat16),
            pltpu.VMEM((steps, half, slots, inner), jnp.bfloat16),
            pltpu.VMEM(norm.shape, jnp.bfloat16),
            dma(),
            dma(members, HALVES),
            dma(steps),
            dma(steps),
            dma(),
        ],
        out_shape=jax.ShapeDtypeStruct((members, points, width), jnp.float32),
        cost_estimate=pl.CostEstimate(
            flops=2 * rows * (block * width + width * inner + inner * channels),
            bytes_accessed=members * points * width * 4 + rows * (inner * 2 + channels * 2),
            transcendentals=0,
        ),
        name="backward",
    )(picks, w_in, w_out, grad, slope, norm)


def swap_members(value):
    return lax.ppermute(value, "member", [(0, 1), (1, 0)])


def to_owners(value):
    return lax.all_to_all(value, GRID, split_axis=0, concat_axis=0, tiled=True)


def device_step(latent, block_pick, obs_weight, obs_value, obs_count, w_in, b_in, w_out, b_out):
    members, points, _ = latent.shape
    peers = lax.axis_size(GRID)
    slots, channels = obs_value.shape[2:]
    members_all = members * lax.axis_size("member")
    picks = block_pick[0]
    counts = obs_count[0]
    weight = to_owners(obs_weight[0])
    live_here = jnp.sum(jnp.minimum(counts, slots)).astype(jnp.float32)
    info = jnp.stack(
        [
            jnp.broadcast_to(counts.astype(jnp.float32)[:, None], (peers, channels)),
            jnp.broadcast_to(live_here, (peers, channels)),
        ],
        axis=1,
    )
    info = jnp.pad(info, ((0, 0), (0, 6), (0, 0)))
    payload = jnp.concatenate([obs_value[0], info], axis=1)
    payload = to_owners(payload)
    own, slope, norm = forward_call(
        picks, latent, weight, w_in, b_in[None], w_out, b_out[None]
    )
    scale = float(peers * peers * slots)
    grad, loss = score_call(own, swap_members(own), payload, members_all, scale)
    loss_all = to_owners(loss)
    loss_value = jnp.sum(loss_all[:, 0, :])
    latent_grad = backward_call(picks, grad, slope, norm, w_in, w_out, points)
    return latent_grad, loss_value


def solution(mesh):
    split = Mesh(
        mesh.devices.reshape(mesh.shape["member"], 4, 4, 4),
        ("member", "grid_0", "grid_1", "grid_2"),
    )
    return jax.shard_map(
        device_step,
        mesh=split,
        in_specs=(
            P("member", GRID, None),
            P(GRID, None),
            P(GRID, None, None, None),
            P(GRID, None, None, None),
            P(GRID, None),
            P(),
            P(),
            P(),
            P(),
        ),
        out_specs=(P("member", GRID, None), P()),
        check_vma=False,
    )
```
